32 devices in a mesh: tm: 2 (over y), row: 4 (over z), col: 4 (over x, core).
Axes of the slice: x: 2, y: 2, z: 4, core: 2. Of those that a mesh axis runs over, the one named last changes fastest.
Arguments:
- returns: bfloat16 [272, 16384], P('tm', ('row', 'col')), may hold values from -60 to 60
- window: int32 [1], replicated, may hold values from 200 to 256
- out_days: int32 [4], replicated, may hold values from 255 to 271
Outputs:
- correlation: bfloat16 [4, 16384, 16384], P(None, 'row', ('col', 'tm'))
The draws below stay inside these ranges and needn't reach their ends.
Inputs may be any that keep to these rules, and one draw needn't show every extreme that they name: One window length for all days. `out_days`: days may repeat.
All inputs are finite; a program needn't handle non-finite values.
Results may differ from the reference program's by a relative error of at most 0.001.
Values may be sent and summed in bfloat16 or wider, within the bound.
A program may use at most 128 MiB of HBM per device.

```python
import jax
import jax.numpy as jnp
from jax import lax

ASSETS = 16384
DAYS = 272
NOUT = 4


def draw_returns(key, part):
    keys = jax.random.split(jax.random.fold_in(key, 17), 5)
    day_scale = jnp.exp(jax.random.uniform(keys[0], (DAYS, 1), jnp.float32, jnp.log(0.3), jnp.log(3.0)))
    asset_scale = jnp.exp(jax.random.uniform(keys[1], (1, ASSETS), jnp.float32, jnp.log(0.5), jnp.log(5.0)))
    loading = jax.random.uniform(keys[2], (1, ASSETS), jnp.float32, 0.4, 1.6)
    market = jax.random.normal(keys[3], (DAYS, 1), jnp.float32)
    noise = jax.random.normal(keys[4], (DAYS, ASSETS), jnp.float32)
    signal = loading * market + noise
    values = jnp.clip(day_scale * asset_scale * signal, -60.0, 60.0)
    return values.astype(jnp.bfloat16)


def plant(entries, key, smallest, top_value):
    extent = entries.shape
    place = [jax.random.randint(jax.random.fold_in(key, axis), (), 0, extent[axis]) for axis in range(len(extent))]
    entries = entries.at[tuple(place)].set(smallest)
    longest = extent.index(max(extent))
    place[longest] = (place[longest] + 1) % extent[longest]
    return entries.at[tuple(place)].set(top_value)


def setup_inputs(seed: int = 0) -> dict:
    streams_of = jax.random.split(jax.random.key(seed), 4)
    return {
        "returns": draw_returns(jax.random.fold_in(streams_of[3], 71), 0),
        "window": jax.random.randint(streams_of[1], (1,), 200, 257).astype(jnp.int32),
        "out_days": plant(jax.random.randint(streams_of[2], (NOUT,), 255, DAYS), jax.random.fold_in(streams_of[2], 1), 255, DAYS - 1).astype(jnp.int32),
    }


def reference(returns, window, out_days):
    width = window[0]
    wide = width.astype(jnp.float32)
    day_ids = jnp.arange(DAYS, dtype=jnp.int32)
    inside = (day_ids[None, :] <= out_days[:, None]) & (day_ids[None, :] > out_days[:, None] - width)
    mask = jnp.where(inside, 1.0, 0.0).astype(jnp.float32)
    series = returns.astype(jnp.float32)
    first = jnp.dot(mask, series, precision=lax.Precision.HIGHEST)
    second = jnp.dot(mask, series * series, precision=lax.Precision.HIGHEST)
    scale = lax.rsqrt((second - first * first / wide) / wide + 1e-06)
    blocks = ASSETS // 512

    def one_block(index):
        start = (index * 512).astype(jnp.int32)
        rows = lax.dynamic_slice_in_dim(series, start, 512, 1)
        weighted = mask[:, :, None] * rows[None, :, :]
        gram = jnp.einsum('kda,db->kab', weighted, series, precision=lax.Precision.HIGHEST)
        first_rows = lax.dynamic_slice_in_dim(first, start, 512, 1)
        scale_rows = lax.dynamic_slice_in_dim(scale, start, 512, 1)
        cov = gram - first_rows[:, :, None] * first[:, None, :] / wide
        return (cov * scale_rows[:, :, None] * scale[:, None, :] / wide).astype(jnp.bfloat16)
    pieces = lax.map(one_block, jnp.arange(blocks, dtype=jnp.int32))
    return jnp.transpose(pieces, (1, 0, 2, 3)).reshape(NOUT, ASSETS, ASSETS)
```

```python
import functools

import jax
import jax.numpy as jnp
from jax import lax
from jax.experimental import pallas as pl
from jax.experimental.pallas import tpu as pltpu
from jax.sharding import PartitionSpec as P

MESH = pl.DeviceIdType.MESH


def gather_kernel(T, R, C, x_ref, row_ref, col_ref, line, line_send, line_recv,
                  row_send, row_recv, twin_send, twin_recv, col_send, col_recv, local_sem):
    t, r, c = lax.axis_index("tm"), lax.axis_index("row"), lax.axis_index("col")
    n = R // T
    core = lax.rem(c, 2)
    twin = c + 1 - 2 * core
    chips = C // 2

    def to(tt, rr, cc):
        return {"tm": tt, "row": rr, "col": cc}

    barrier = pltpu.get_barrier_semaphore()
    for d in range(1, T * C):
        flat = lax.rem(t * C + c + d, T * C)
        pl.semaphore_signal(barrier, inc=1, device_id=to(flat // C, r, lax.rem(flat, C)), device_id_type=MESH)

    @pl.when(r > 0)
    def _():
        pl.semaphore_signal(barrier, inc=1, device_id=to(t, r - 1, c), device_id_type=MESH)

    @pl.when(r < R - 1)
    def _():
        pl.semaphore_signal(barrier, inc=1, device_id=to(t, r + 1, c), device_id_type=MESH)

    inner = jnp.logical_and(r > 0, r < R - 1)
    pl.semaphore_wait(barrier, T * C + inner.astype(jnp.int32) if R > 1 else T * C - 1)

    def rdma(src, dst, send, recv, device):
        return pltpu.make_async_remote_copy(src_ref=src, dst_ref=dst, send_sem=send, recv_sem=recv,
                                            device_id=device, device_id_type=MESH)

    def line_copy(src, q, up):
        return rdma(src, line.at[q], line_send.at[int(up), q], line_recv.at[q],
                    to(t, r + (1 if up else -1), c))

    def send_line(src, q, up):
        ok = (r < R - 1) if up else (r > 0)

        @pl.when(ok)
        def _():
            line_copy(src, q, up).start()

    def col_place(q):
        piece = q * C + c
        group = piece // n
        return lax.rem(group, T), group // T, lax.rem(piece, n)

    def col_copy(src, q):
        tt, cc, j = col_place(q)
        return rdma(src, col_ref.at[t, j], col_send.at[q], col_recv.at[t, j], to(tt, r, cc))

    def send_col(src, q):
        tt, cc, j = col_place(q)
        mine = jnp.logical_and(tt == t, cc == c)

        @pl.when(mine)
        def _():
            pltpu.make_async_copy(src, col_ref.at[t, j], col_recv.at[t, j]).start()

        @pl.when(jnp.logical_not(mine))
        def _():
            col_copy(src, q).start()

    own_out = pltpu.make_async_copy(x_ref, row_ref.at[t, c], local_sem)
    send_line(x_ref, r, True)
    send_line(x_ref, r, False)

    def row_copy(d):
        flat = lax.rem(t * chips + c // 2 + d, T * chips)
        return rdma(x_ref, row_ref.at[t, c], row_send.at[d], row_recv.at[d],
                    to(flat // chips, r, 2 * lax.rem(flat, chips) + core))

    for d in range(1, T * chips):
        row_copy(d).start()
    rdma(x_ref, row_ref.at[t, c], twin_send.at[0], twin_recv.at[0], to(t, r, twin)).start()
    own_out.start()
    send_col(x_ref, r)

    def row_arrived(d):
        flat = lax.rem(t * chips + c // 2 - d + T * chips, T * chips)
        slot = row_ref.at[flat // chips, 2 * lax.rem(flat, chips) + core]
        rdma(slot, slot, row_send.at[d], row_recv.at[d], to(t, r, twin)).wait_recv()
        rdma(slot, slot, twin_send.at[d], twin_recv.at[d], to(t, r, twin)).start()

    def line_arrived(dist):
        for up in (True, False):
            q = r - dist if up else r + dist
            ok = (q >= 0) if up else (q < R)

            @pl.when(ok)
            def _():
                line_copy(line.at[q], q, up).wait_recv()
                send_line(line.at[q], q, up)
                send_col(line.at[q], q)

    for dist in range(1, R):
        line_arrived(dist)
        if dist == 1:
            for d in range(1, T * chips):
                row_arrived(d)

    own_out.wait()
    for d in range(1, T * chips):
        row_copy(d).wait_send()
    for d in range(T * chips):
        flat = lax.rem(t * chips + c // 2 - d + T * chips, T * chips)
        mine = row_ref.at[flat // chips, 2 * lax.rem(flat, chips) + core]
        theirs = row_ref.at[flat // chips, 2 * lax.rem(flat, chips) + 1 - core]
        rdma(mine, mine, twin_send.at[d], twin_recv.at[d], to(t, r, twin)).wait_send()
        rdma(theirs, theirs, twin_send.at[d], twin_recv.at[d], to(t, r, twin)).wait_recv()
    for tt in range(T):
        for j in range(n):
            slot = col_ref.at[tt, j]
            pltpu.make_async_copy(slot, slot, col_recv.at[tt, j]).wait()
    for q in range(R):
        tt, cc, j = col_place(q)

        @pl.when(jnp.logical_not(jnp.logical_and(tt == t, cc == c)))
        def _():
            col_copy(x_ref, q).wait_send()

        @pl.when(jnp.logical_and(q <= r, r < R - 1))
        def _():
            line_copy(x_ref, q, True).wait_send()

        @pl.when(jnp.logical_and(q >= r, r > 0))
        def _():
            line_copy(x_ref, q, False).wait_send()


def gather(returns, T, R, C):
    days, width = returns.shape
    n = R // T
    dma = pltpu.SemaphoreType.DMA
    chips = T * C // 2
    return pl.pallas_call(
        functools.partial(gather_kernel, T, R, C),
        out_shape=(
            jax.ShapeDtypeStruct((T, C, days, width), returns.dtype),
            jax.ShapeDtypeStruct((T, n, days, width), returns.dtype),
        ),
        in_specs=[pl.BlockSpec(memory_space=pltpu.VMEM)],
        out_specs=(pl.BlockSpec(memory_space=pl.ANY), pl.BlockSpec(memory_space=pl.ANY)),
        scratch_shapes=[
            pltpu.VMEM((R, days, width), returns.dtype),
            dma((2, R)), dma((R,)),
            dma((chips,)), dma((chips,)),
            dma((chips,)), dma((chips,)),
            dma((R,)), dma((T, n)), dma,
        ],
        compiler_params=pltpu.CompilerParams(collective_id=0, has_side_effects=True),
    )(returns)


def corr_kernel(tile, depth, window_ref, out_ref_days, row_ref, col_ref, o_ref,
                rows_t, cols, col_a, col_m):
    i, k = pl.program_id(0), pl.program_id(1)
    K = out_ref_days.shape[0]
    T, n, half_days, width = col_ref.shape
    days = T * half_days
    extra = days - depth
    w = window_ref[0]
    wide = w.astype(jnp.float32)
    recip = 1.0 / wide

    def slot_mask(shape, dim, last):
        s = lax.broadcasted_iota(jnp.int32, shape, dim)
        day = jnp.where(s + depth <= last, s + depth, s)
        return (day <= last) & (day > last - w)

    def joined(ref, at):
        return jnp.concatenate([ref[tt, at] for tt in range(T)], axis=0)

    @pl.when((i == 0) & (k == 0))
    def _():
        for j in range(n):
            x = joined(col_ref, j)
            at = pl.ds(j * width, width)
            for kk in range(K):
                last = out_ref_days[kk]
                slot = lax.broadcasted_iota(jnp.int32, (extra, width), 0)
                head = jnp.where(slot + depth <= last, x[depth:].astype(jnp.float32),
                                 x[:extra].astype(jnp.float32)).astype(x.dtype)
                cols[kk, :extra, at] = head
                cols[kk, extra:, at] = x[extra:depth]
                f = jnp.where(slot_mask((depth, width), 0, last),
                              cols[kk, :, at].astype(jnp.float32), 0.0)
                first = jnp.sum(f, axis=0, keepdims=True)
                second = jnp.sum(f * f, axis=0, keepdims=True)
                scale = lax.rsqrt((second - first * first / wide) / wide + 1e-06)
                col_a[kk, :, at] = scale * recip
                col_m[kk, :, at] = first * recip * (scale * recip)

    per_piece = width // tile if width >= tile else 1

    @pl.when(k == 0)
    def _():
        piece = i // per_piece
        at = pl.ds(pl.multiple_of(lax.rem(i, per_piece) * tile, 128), tile)
        x = jnp.concatenate([row_ref[tt, piece, :, at] for tt in range(T)], axis=0)
        rows_t[:, :depth] = x[:depth].T
        tail = jnp.concatenate([x[depth:], jnp.zeros((128 - extra, tile), x.dtype)], axis=0)
        rows_t[:, depth:] = tail.T

    last = out_ref_days[k]
    lane = lax.broadcasted_iota(jnp.int32, (tile, 128), 1)
    use = (lane < extra) & (lane + depth <= last)
    head = jnp.where(use, rows_t[:, depth:].astype(jnp.float32), rows_t[:, :128].astype(jnp.float32))
    f = jnp.concatenate([head, rows_t[:, 128:depth].astype(jnp.float32)], axis=1)
    f = jnp.where(slot_mask((tile, depth), 1, last), f, 0.0)
    lhs = f.astype(jnp.bfloat16)
    first = jnp.sum(f, axis=1, keepdims=True)
    second = jnp.sum(f * f, axis=1, keepdims=True)
    scale = lax.rsqrt((second - first * first / wide) / wide + 1e-06)
    m = first * scale
    N = cols.shape[2]
    step = 256 if N % 256 == 0 else 128
    for b in range(0, N, step):
        g = jnp.dot(lhs, cols[k, :, b:b + step], preferred_element_type=jnp.float32)
        o = (g * scale) * col_a[k, :, b:b + step] - m * col_m[k, :, b:b + step]
        o_ref[0, :, b:b + step] = o.astype(o_ref.dtype)


def correlate(window, out_days, rows, cols):
    T, C, half_days, width = rows.shape
    n = cols.shape[1]
    K = out_days.shape[0]
    M, N = C * width, n * width
    depth = 256
    tile = min(512, width)
    grid_spec = pltpu.PrefetchScalarGridSpec(
        num_scalar_prefetch=2,
        grid=(M // tile, K),
        in_specs=[
            pl.BlockSpec(rows.shape, lambda i, k, *_: (0, 0, 0, 0)),
            pl.BlockSpec(cols.shape, lambda i, k, *_: (0, 0, 0, 0)),
        ],
        out_specs=pl.BlockSpec((1, tile, N), lambda i, k, *_: (k, i, 0)),
        scratch_shapes=[
            pltpu.VMEM((tile, depth + 128), jnp.bfloat16),
            pltpu.VMEM((K, depth, N), jnp.bfloat16),
            pltpu.VMEM((K, 1, N), jnp.float32),
            pltpu.VMEM((K, 1, N), jnp.float32),
        ],
    )
    return pl.pallas_call(
        functools.partial(corr_kernel, tile, depth),
        out_shape=jax.ShapeDtypeStruct((K, M, N), jnp.bfloat16),
        grid_spec=grid_spec,
        compiler_params=pltpu.CompilerParams(
            dimension_semantics=("arbitrary", "arbitrary"), vmem_limit_bytes=60 * 2**20),
    )(window, out_days, rows, cols)


def on_device(returns, window, out_days):
    T, R, C = lax.axis_size("tm"), lax.axis_size("row"), lax.axis_size("col")
    rows, cols = gather(returns, T, R, C)
    return correlate(window, out_days, rows, cols)


def solution(mesh):
    return jax.shard_map(
        on_device,
        mesh=mesh,
        in_specs=(P("tm", ("row", "col")), P(), P()),
        out_specs=P(None, "row", ("col", "tm")),
        check_vma=False,
    )
```
